32 devices in a mesh: tm: 8 (over z, x), space: 4 (over y, core).
Axes of the slice: x: 2, y: 2, z: 4, core: 2. Of those that a mesh axis runs over, the one named last changes fastest.
Arguments:
- snapshots: bfloat16 [1024, 73728], P('tm', 'space'), may hold values from -12 to 12
- start_block: float32 [1024, 20], P('tm'), may hold values from -6 to 6
- merge_mix: float32 [40, 20], replicated, may hold values from -1 to 1
Outputs:
- modes: float32 [20, 73728], P(None, ('space', 'tm'))
- spectrum: float32 [20], replicated
The draws below stay inside these ranges and needn't reach their ends.
All inputs are finite; a program needn't handle non-finite values.
Results may differ from the reference program's by a relative error of at most 0.012.
Values sent between devices are 32-bit elements; how exact they have to be, the bound alone decides.
No kernel may reach another device: no remote copies, remote signals or barrier semaphores. Data moves between devices by JAX's collectives and lax.ppermute only.
A program may use at most 64 MiB of HBM per device.

```python
import math
import jax
import jax.numpy as jnp
from jax import lax

R = 20
SNAP_DEV = 128
WIDTH = 73728
ITERS = 2
LEVELS = 3
SNAPSHOTS = 1024
N_TM = 8


def draw_snapshots(key, part):
    keys = jax.random.split(jax.random.fold_in(key, 7), 3)
    steps = jnp.arange(R, dtype=jnp.float32)
    shared_decay = 0.95 ** steps
    own_decay = 0.7 * 0.95 ** steps
    shared_shapes = jax.random.normal(keys[0], (R, WIDTH), jnp.float32)
    rough = jnp.exp(jax.random.uniform(keys[1], (1, WIDTH), jnp.float32, math.log(0.7), math.log(1.4)))
    ramp = jnp.exp(jnp.linspace(math.log(0.5), math.log(2.0), WIDTH, dtype=jnp.float32))[None, :]
    col_scale = ramp * rough

    def one_tile(index):
        tile_keys = jax.random.split(jax.random.fold_in(keys[2], index), 4)
        shared_w = jax.random.normal(tile_keys[0], (SNAP_DEV, R), jnp.float32) * shared_decay
        own_w = jax.random.normal(tile_keys[1], (SNAP_DEV, R), jnp.float32) * own_decay
        own_shapes = jax.random.normal(tile_keys[2], (R, WIDTH), jnp.float32)
        noise = jax.random.normal(tile_keys[3], (SNAP_DEV, WIDTH), jnp.float32)
        values = jnp.dot(shared_w, shared_shapes, precision=lax.Precision.HIGHEST)
        values = values + jnp.dot(own_w, own_shapes, precision=lax.Precision.HIGHEST) + 0.1 * noise
        values = values * col_scale
        return jnp.clip(values, -12.0, 12.0).astype(jnp.bfloat16)
    tiles = lax.map(one_tile, jnp.arange(SNAPSHOTS // SNAP_DEV, dtype=jnp.int32))
    return tiles.reshape(SNAPSHOTS, WIDTH)


def levels(stream_key, extent, cuts, least, top_value):
    def one(axis_at, shards_of):
        steps = jax.random.uniform(jax.random.fold_in(jax.random.fold_in(stream_key, 6), axis_at), (shards_of,), jnp.float32, least / len(cuts), top_value / len(cuts))
        return jnp.repeat(jnp.exp(steps), extent[axis_at] // shards_of).reshape((-1,) + (1,) * (len(extent) - axis_at - 1))

    loudness = one(*cuts[0])
    for cut in cuts[1:]:
        loudness = loudness * one(*cut)
    return loudness


def centred(own_key, extent, deviation, limit, cuts=(), held_as=jnp.bfloat16):
    array = deviation * jax.random.normal(own_key, extent, jnp.float32)
    if cuts:
        array = array * levels(own_key, extent, cuts, -0.22, 0.18)
    return jnp.clip(array, -limit, limit).astype(held_as)


def setup_inputs(seed: int = 0) -> dict:
    key_list = jax.random.split(jax.random.key(seed), 4)
    snapshots = draw_snapshots(jax.random.fold_in(key_list[3], 71), 0)
    start_block = centred(key_list[1], (SNAPSHOTS, R), 1.0, 6.0, ((0, 8),), jnp.float32)
    merge_mix = centred(key_list[2], (2 * R, R), (2 * R) ** -0.5, 1.0, (), jnp.float32)
    return {"snapshots": snapshots, "start_block": start_block, "merge_mix": merge_mix}


HIGHEST_PREC = lax.Precision.HIGHEST

def merge_rule(gram_mat, mixing):
    weighted = jnp.dot(gram_mat, mixing, precision=HIGHEST_PREC)
    small_gram = jnp.dot(mixing.T, weighted, precision=HIGHEST_PREC)
    cholesky_low = jnp.linalg.cholesky(small_gram)
    coef_map = jax.scipy.linalg.solve_triangular(cholesky_low, mixing.T, lower=True)
    spread = jnp.dot(coef_map, gram_mat, precision=HIGHEST_PREC)
    singular = jnp.sqrt(lax.optimization_barrier(jnp.sum(spread * spread, axis=1)))
    return (coef_map, singular)

def tile_factor(window, start):
    block_proj = start
    for rounds in range(ITERS):
        rounded = block_proj.astype(jnp.bfloat16)
        images = jnp.dot(rounded.T.astype(jnp.float32), window.astype(jnp.float32), preferred_element_type=jnp.float32)
        images_b = images.astype(jnp.bfloat16)
        gram_mat = jnp.dot(images_b.astype(jnp.float32), images_b.T.astype(jnp.float32), preferred_element_type=jnp.float32)
        projected = jnp.dot(window.astype(jnp.float32), images_b.T.astype(jnp.float32), preferred_element_type=jnp.float32)
        cholesky_low = jnp.linalg.cholesky(gram_mat)
        block_proj = jax.scipy.linalg.solve_triangular(cholesky_low, projected.T, lower=True).T
    singular = jnp.sqrt(lax.optimization_barrier(jnp.sum(block_proj * block_proj, axis=0)))
    basis_rows = jax.scipy.linalg.solve_triangular(cholesky_low, images_b.astype(jnp.float32), lower=True)
    return singular[:, None] * basis_rows

def reference(snapshots, start_block, merge_mix):
    windows = snapshots.reshape(N_TM, SNAP_DEV, WIDTH)
    starts = start_block.reshape(N_TM, SNAP_DEV, R)
    factors = lax.map(lambda pieces: tile_factor(pieces[0], pieces[1]), (windows, starts))
    for height in range(LEVELS):
        pair_count = factors.shape[0] // 2
        stacked = factors.reshape(pair_count, 2 * R, WIDTH)
        gram_mat = jnp.einsum('gam,gbm->gab', stacked, stacked, precision=HIGHEST_PREC)
        coef_map, singular = jax.vmap(merge_rule, in_axes=(0, None))(gram_mat, merge_mix)
        basis_rows = jnp.einsum('grk,gkm->grm', coef_map, stacked, precision=HIGHEST_PREC)
        factors = singular[:, :, None] * basis_rows
    modes = basis_rows[0] * math.sqrt(WIDTH)
    spectrum = singular[0] / math.sqrt(SNAP_DEV * WIDTH)
    return (modes, spectrum)
```

```python
import functools
import math

import jax
import jax.numpy as jnp
from jax import lax
from jax.experimental import pallas as pl
from jax.experimental.pallas import tpu as pltpu
from jax.sharding import PartitionSpec as P

ITERS = 2
LANES = 128
SUBLANES = 8
EYE_LANE = 32

HIGHEST_PREC = lax.Precision.HIGHEST


def from_partner(block, axis, distance):
    count = lax.axis_size(axis)
    route = []
    for low in range(count):
        high = low | 1 << distance
        if high != low and high < count:
            route += [(low, high), (high, low)]
    return lax.ppermute(block, axis, route)


def merge_rule(gram_mat, mixing):
    weighted = jnp.dot(gram_mat, mixing, precision=HIGHEST_PREC)
    small_gram = jnp.dot(mixing.T, weighted, precision=HIGHEST_PREC)
    cholesky_low = jnp.linalg.cholesky(small_gram)
    coef_map = jax.scipy.linalg.solve_triangular(cholesky_low, mixing.T, lower=True)
    spread = jnp.dot(coef_map, gram_mat, precision=HIGHEST_PREC)
    singular = jnp.sqrt(jnp.sum(spread * spread, axis=1))
    return (coef_map, singular)


def local_plain(snapshots, start_block, merge_mix):
    width = snapshots.shape[1] * lax.axis_size("space")
    block_proj = start_block
    for rounds in range(ITERS):
        rounded = block_proj.astype(jnp.bfloat16)
        images = lax.dot_general(
            rounded, snapshots, (((0,), (0,)), ((), ())), preferred_element_type=jnp.float32
        )
        images_b = images.astype(jnp.bfloat16)
        gram_part = lax.dot_general(
            images_b, images_b, (((1,), (1,)), ((), ())), preferred_element_type=jnp.float32
        )
        proj_part = lax.dot_general(
            snapshots, images_b, (((1,), (1,)), ((), ())), preferred_element_type=jnp.float32
        )
        gram_mat, projected = lax.psum((gram_part, proj_part), "space")
        cholesky_low = jnp.linalg.cholesky(gram_mat)
        block_proj = jax.scipy.linalg.solve_triangular(cholesky_low, projected.T, lower=True).T
    singular = jnp.sqrt(jnp.sum(block_proj * block_proj, axis=0))
    basis_rows = jax.scipy.linalg.solve_triangular(
        cholesky_low, images_b.astype(jnp.float32), lower=True
    )
    factor = singular[:, None] * basis_rows
    tile_total = lax.axis_size("tm")
    depth_total = tile_total.bit_length() - 1
    tm_place = lax.axis_index("tm")
    for height in range(depth_total):
        partner = from_partner(factor, "tm", height)
        upper = tm_place >> height & 1 == 1
        first = jnp.where(upper, partner, factor)
        second = jnp.where(upper, factor, partner)
        stacked = jnp.concatenate([first, second], axis=0)
        gram_local = jnp.dot(stacked, stacked.T, precision=HIGHEST_PREC)
        gram_mat = lax.psum(gram_local, "space")
        coef_map, singular = merge_rule(gram_mat, merge_mix)
        basis_rows = jnp.dot(coef_map, stacked, precision=HIGHEST_PREC)
        factor = singular[:, None] * basis_rows
    piece_cols = basis_rows.shape[1] // tile_total
    own_cols = lax.dynamic_slice_in_dim(basis_rows, tm_place * piece_cols, piece_cols, 1)
    modes = own_cols * math.sqrt(width)
    spectrum = singular / math.sqrt(snapshots.shape[0] * width)
    return (modes, spectrum)


def mm(a, b, dims=((1,), (0,))):
    return lax.dot_general(
        a, b, (dims, ((), ())), precision=HIGHEST_PREC, preferred_element_type=jnp.float32
    )


def iota(shape, dim):
    return lax.broadcasted_iota(jnp.int32, shape, dim)


def one_hot(cond):
    return jnp.where(cond, 1.0, 0.0).astype(jnp.float32)


def spread_map(rows, cols, step):
    return one_hot(iota((rows, cols), 1) % step == iota((rows, cols), 0))


def block_mask(shape, row_step, col_step):
    return iota(shape, 0) // row_step == iota(shape, 1) // col_step


def with_eye(gram_mat, rank):
    row = iota(gram_mat.shape, 0)
    lane = iota(gram_mat.shape, 1)
    return jnp.where(lane < rank, gram_mat, one_hot((lane == row + EYE_LANE) & (row < rank)))


def eliminate(systems, rank):
    systems = [list(s) for s in systems]
    row = iota((systems[0][0].shape[0], 1), 0)
    for k in range(rank - 1):
        for s in systems:
            a = s[0]
            scale = a[:, k : k + 1] / a[k : k + 1, k : k + 1]
            scale = jnp.where(row > k, scale, 0.0)
            for i, v in enumerate(s):
                s[i] = v - scale * v[k : k + 1, :]
    out = []
    for s in systems:
        a = s[0]
        at_diag = iota(a.shape, 0) == iota(a.shape, 1)
        pivots = jnp.sum(jnp.where(at_diag, a, 0.0), axis=1, keepdims=True)
        inv = jnp.where(row < rank, lax.rsqrt(jnp.where(row < rank, pivots, 1.0)), 0.0)
        out.append([v * inv for v in s])
    return out


def roll_lanes(x, shift):
    return pltpu.roll(x, shift % x.shape[1], 1)


def head_body(*refs, rank, rank_pad):
    *corr_refs, start_ref, proj_ref, slab_ref = refs
    corr = corr_refs[0][...]
    for ref in corr_refs[1:]:
        corr = corr + ref[...]
    snaps = corr.shape[0]
    start = start_ref[...]
    wide = jnp.concatenate([start, jnp.zeros((snaps, LANES - rank), jnp.float32)], axis=1)
    block_t = wide.T
    for rounds in range(ITERS):
        rounded = block_t.astype(jnp.bfloat16).astype(jnp.float32)
        proj_t = mm(rounded[:rank_pad], corr)
        gram_mat = mm(proj_t, rounded, ((1,), (1,)))
        ((done, solved),) = eliminate([(with_eye(gram_mat, rank), proj_t)], rank)
        block_t = jnp.concatenate(
            [solved, jnp.zeros((LANES - rank_pad, snaps), jnp.float32)], axis=0
        )
    proj_ref[...] = rounded[:rank_pad].astype(jnp.bfloat16)
    singular = jnp.sqrt(jnp.sum(solved * solved, axis=1, keepdims=True))
    factor_map = singular * done
    lane = iota(factor_map.shape, 1)
    factor_map = jnp.where((lane >= EYE_LANE) & (lane < EYE_LANE + rank), factor_map, 0.0)
    slab = jnp.zeros((SUBLANES, LANES), jnp.float32)
    for q in range(rank_pad // SUBLANES):
        part = factor_map[q * SUBLANES : (q + 1) * SUBLANES]
        slab = slab + roll_lanes(part, q * rank_pad - EYE_LANE)
    slab_ref[...] = slab


def image_body(place_ref, proj_ref, slab_ref, snap_ref, *out_refs, rank, rank_pad):
    piece = snap_ref.shape[1]
    half = piece // 2
    full = rank // SUBLANES
    images = jnp.dot(proj_ref[...], snap_ref[...], preferred_element_type=jnp.float32)
    images = images.astype(jnp.bfloat16).astype(jnp.float32)
    for d, out_ref in enumerate(out_refs):

        @pl.when(pl.program_id(0) == d)
        def _():
            for q in range(full):
                out_ref[:, q * piece : (q + 1) * piece] = images[q * SUBLANES : (q + 1) * SUBLANES]
            rest = images[full * SUBLANES : rank_pad]
            low = rest[:, :half]
            high = pltpu.roll(rest[:, half:], SUBLANES // 2, 0)
            out_ref[:, full * piece : full * piece + half] = low + high
            out_ref[:, full * piece + half :] = slab_ref[...]


def mix_body(mix_ref, wide_ref, pair_ref, *, rank, rank_pad):
    wide_ref[...] = jnp.zeros(wide_ref.shape, jnp.float32)
    wide_ref[0:rank, 0:rank] = mix_ref[0:rank, :]
    wide_ref[rank_pad : rank_pad + rank, 0:rank] = mix_ref[rank : 2 * rank, :]
    pairs = pair_ref.shape[0] // (2 * rank_pad)
    spread = mm(wide_ref[...], spread_map(LANES, LANES, rank_pad))
    stacked = jnp.concatenate([spread] * pairs, axis=0)
    pair_ref[...] = jnp.where(block_mask(stacked.shape, 2 * rank_pad, rank_pad), stacked, 0.0)


def gram_body(place_ref, *refs, tiles, rank, rank_pad):
    piece_refs = refs[:tiles]
    pair_ref, part_ref, rows_ref, span_ref, rows_f32, map_ref = refs[tiles:]
    piece = rows_f32.shape[1]
    half = piece // 2
    full = rank // SUBLANES
    place = place_ref[0]
    lane8 = iota((SUBLANES, LANES), 1)
    row8 = iota((SUBLANES, half), 0)
    for d in range(tiles):
        tile_row = pl.multiple_of((place ^ d) * rank_pad, SUBLANES)
        ref = piece_refs[d]
        for q in range(full):
            at = pl.ds(pl.multiple_of(tile_row + q * SUBLANES, SUBLANES), SUBLANES)
            rows_f32[at, :] = ref[:, q * piece : (q + 1) * piece]
        rest = ref[:, full * piece : full * piece + half]
        at = pl.ds(pl.multiple_of(tile_row + full * SUBLANES, SUBLANES), SUBLANES)
        rows_f32[at, 0:half] = jnp.where(row8 < SUBLANES // 2, rest, 0.0)
        rest = pltpu.roll(rest, SUBLANES // 2, 0)
        rows_f32[at, half:] = jnp.where(row8 < SUBLANES // 2, rest, 0.0)
        slab = ref[:, full * piece + half :]
        for q in range(rank_pad // SUBLANES):
            at = pl.ds(pl.multiple_of(tile_row + q * SUBLANES, SUBLANES), SUBLANES)
            map_ref[at, :] = jnp.where(lane8 < rank, roll_lanes(slab, -q * rank_pad), 0.0)
    rows = rows_f32[...].astype(jnp.bfloat16)
    rows_ref[...] = rows
    gram_mat = lax.dot_general(
        rows, rows, (((1,), (1,)), ((), ())), preferred_element_type=jnp.float32
    )
    total = tiles * rank_pad
    pairs = tiles // 2
    used = pairs * rank_pad
    maps = mm(map_ref[...], spread_map(LANES, total, rank_pad))
    maps = jnp.where(block_mask(maps.shape, rank_pad, rank_pad), maps, 0.0)
    pair = pair_ref[...]
    span = mm(pair, maps, ((0,), (0,)))[:used]
    span_ref[...] = span
    cross = mm(mm(span, gram_mat), maps, ((1,), (1,)))
    mixed = mm(cross, pair)
    own = jnp.where(block_mask(cross.shape, rank_pad, 2 * rank_pad), cross, 0.0)
    src = iota((total, LANES), 0)
    dst = iota((total, LANES), 1)
    inner = src % (2 * rank_pad)
    target = jnp.where(
        inner < rank_pad, src // (2 * rank_pad) * rank_pad + inner, used + inner - rank_pad
    )
    moved = mm(own, one_hot(dst == target))
    outside = ~block_mask(mixed.shape, rank_pad, rank_pad)
    part_ref[...] = jnp.where(outside, mixed, 0.0) + moved


def tree_body(*refs, parts, rank, rank_pad, tiles, mode_scale, value_scale):
    part_refs = refs[:parts]
    wide_ref, pair_ref, span_ref, rows_ref, modes_ref, spectrum_ref = refs[parts:]
    part = part_refs[0][...]
    for ref in part_refs[1:]:
        part = part + ref[...]
    count = tiles // 2
    used = count * rank_pad
    wide = wide_ref[...]
    wide = jnp.concatenate(
        [wide, jnp.zeros((LANES - 2 * rank_pad, LANES), jnp.float32)], axis=0
    )
    lane = iota((rank_pad, LANES), 1)
    blocks = []
    for b in range(count):
        mine = part[b * rank_pad : (b + 1) * rank_pad]
        first = jnp.where(lane < rank_pad, roll_lanes(mine, -b * rank_pad), 0.0)
        second = jnp.where((lane >= used) & (lane < used + rank_pad), mine, 0.0)
        blocks.append(first + roll_lanes(second, rank_pad - used))
    own = mm(jnp.concatenate(blocks, axis=0), wide)
    grams = [own[b * rank_pad : (b + 1) * rank_pad] for b in range(count)]
    spread = spread_map(LANES, LANES, rank_pad)
    span = span_ref[...]
    outside = ~block_mask(part.shape, rank_pad, rank_pad) & (iota(part.shape, 1) < used)
    diag = block_mask(part.shape, rank_pad, rank_pad)
    full = jnp.where(outside, part, 0.0) + jnp.where(diag, mm(own, spread), 0.0)
    while True:
        systems = []
        for b in range(count):
            if count > 1:
                systems.append((with_eye(grams[b], rank), blocks[b]))
            else:
                systems.append((jnp.where(lane < rank, grams[b], 0.0), blocks[b], span))
        solved = eliminate(systems, rank)
        values = [jnp.sqrt(jnp.sum(s[1] * s[1], axis=1, keepdims=True)) for s in solved]
        if count == 1:
            break
        maps = []
        for b in range(count):
            scaled = roll_lanes(solved[b][0] * values[b], -EYE_LANE)
            maps.append(jnp.where(lane < rank, scaled, 0.0))
        maps = jnp.concatenate(maps, axis=0)
        maps = mm(maps, spread)
        maps = jnp.where(block_mask(maps.shape, rank_pad, rank_pad), maps, 0.0)
        rows_now = count * rank_pad
        count //= 2
        used = count * rank_pad
        pair = pair_ref[0:rows_now, :]
        pair = jnp.where(iota(pair.shape, 1) < used, pair, 0.0)
        step = mm(pair, maps, ((0,), (0,)))[:used]
        half_way = mm(step[:, :rows_now], full[:rows_now])
        pad_rows = jnp.zeros((LANES - rows_now, LANES), jnp.float32)
        maps_full = jnp.concatenate([maps, pad_rows], axis=0) if rows_now < LANES else maps
        cross = mm(half_way, maps_full, ((1,), (1,)))
        step_pad = jnp.concatenate([step, jnp.zeros((LANES - used, LANES), jnp.float32)], axis=0)
        full = mm(half_way, step_pad, ((1,), (1,)))
        span = mm(step[:, :rows_now], span)
        blocks = []
        grams = []
        for b in range(count):
            at = slice(b * rank_pad, (b + 1) * rank_pad)
            first = roll_lanes(cross[at], -2 * b * rank_pad)
            blocks.append(jnp.where(lane < 2 * rank_pad, first, 0.0))
            grams.append(roll_lanes(full[at], -b * rank_pad))
    coef = solved[0][2] * mode_scale
    high = coef.astype(jnp.bfloat16)
    rest = coef - high.astype(jnp.float32)
    mid = rest.astype(jnp.bfloat16)
    low = (rest - mid.astype(jnp.float32)).astype(jnp.bfloat16)
    rows = rows_ref[...]
    modes = jnp.dot(high, rows, preferred_element_type=jnp.float32)
    modes = modes + jnp.dot(mid, rows, preferred_element_type=jnp.float32)
    modes = modes + jnp.dot(low, rows, preferred_element_type=jnp.float32)
    modes_ref[...] = modes[:rank]
    square = solved[0][1] * solved[0][1]
    value_row = jnp.sqrt(mm(jnp.ones((SUBLANES, LANES), jnp.float32), square, ((1,), (1,))))
    spectrum_ref[...] = value_row[0:1, 0:rank] * value_scale


def fits(mesh, snapshots, start_block):
    tiles, spaces = mesh.shape["tm"], mesh.shape["space"]
    rank = start_block.shape[1]
    rank_pad = -(-rank // SUBLANES) * SUBLANES
    snaps = snapshots.shape[0]
    piece = snapshots.shape[1] // tiles
    return (
        tiles & tiles - 1 == 0
        and spaces & spaces - 1 == 0
        and tiles >= 4
        and (tiles // 2 + 1) * rank_pad <= LANES
        and rank % SUBLANES == SUBLANES // 2
        and rank <= EYE_LANE
        and rank + EYE_LANE <= LANES
        and snaps == LANES
        and snapshots.shape[1] % tiles == 0
        and piece % (2 * LANES) == 0
    )


def swap(block, axes, distance):
    size = 1
    for axis in axes:
        size *= lax.axis_size(axis)
    return lax.ppermute(block, axes, [(i, i ^ distance) for i in range(size)])


def local_fast(snapshots, start_block, merge_mix):
    tiles, spaces = lax.axis_size("tm"), lax.axis_size("space")
    snaps, cols = snapshots.shape
    rank = start_block.shape[1]
    rank_pad = -(-rank // SUBLANES) * SUBLANES
    width = cols * spaces
    piece = cols // tiles
    pairs = tiles // 2
    total = tiles * rank_pad
    f32 = jnp.float32
    place = lax.axis_index("tm").astype(jnp.int32).reshape(1)
    sizes = {"rank": rank, "rank_pad": rank_pad}

    wide, pair = pl.pallas_call(
        functools.partial(mix_body, **sizes),
        out_shape=[
            jax.ShapeDtypeStruct((2 * rank_pad, LANES), f32),
            jax.ShapeDtypeStruct((total, LANES), f32),
        ],
        name="mix_maps",
    )(merge_mix)

    corr = lax.dot_general(
        snapshots, snapshots, (((1,), (1,)), ((), ())), preferred_element_type=f32
    )
    corrs = [corr] + [swap(corr, ("space",), d) for d in range(1, spaces)]
    proj, slab = pl.pallas_call(
        functools.partial(head_body, **sizes),
        out_shape=[
            jax.ShapeDtypeStruct((rank_pad, snaps), jnp.bfloat16),
            jax.ShapeDtypeStruct((SUBLANES, LANES), f32),
        ],
        name="tile_iterations",
    )(*corrs, start_block)

    packed = rank * piece // SUBLANES + LANES
    pieces = pl.pallas_call(
        functools.partial(image_body, **sizes),
        grid_spec=pltpu.PrefetchScalarGridSpec(
            num_scalar_prefetch=1,
            grid=(tiles,),
            in_specs=[
                pl.BlockSpec((rank_pad, snaps), lambda d, at: (0, 0)),
                pl.BlockSpec((SUBLANES, LANES), lambda d, at: (0, 0)),
                pl.BlockSpec((snaps, piece), lambda d, at: (0, at[0] ^ d)),
            ],
            out_specs=[pl.BlockSpec((SUBLANES, packed), lambda d, at: (0, 0))] * tiles,
        ),
        out_shape=[jax.ShapeDtypeStruct((SUBLANES, packed), f32)] * tiles,
        compiler_params=pltpu.CompilerParams(dimension_semantics=("arbitrary",)),
        name="images",
    )(place, proj, slab, snapshots)
    got = [pieces[0]] + [swap(pieces[d], ("tm",), d) for d in range(1, tiles)]

    vmem = pl.BlockSpec(memory_space=pltpu.VMEM)
    part, rows, span = pl.pallas_call(
        functools.partial(gram_body, tiles=tiles, **sizes),
        in_specs=[pl.BlockSpec(memory_space=pltpu.SMEM)] + [vmem] * (tiles + 1),
        out_specs=[vmem] * 3,
        out_shape=[
            jax.ShapeDtypeStruct((pairs * rank_pad, LANES), f32),
            jax.ShapeDtypeStruct((total, piece), jnp.bfloat16),
            jax.ShapeDtypeStruct((pairs * rank_pad, total), f32),
        ],
        scratch_shapes=[
            pltpu.VMEM((total, piece), f32),
            pltpu.VMEM((total, LANES), f32),
        ],
        name="cross_gram",
    )(place, *got, pair)

    bits = (tiles * spaces).bit_length() - 1
    start = 0
    parts = [part]
    while start < bits:
        take = 1 if (bits - start) % 2 else 2
        part = sum(parts[1:], parts[0])
        parts = [part] + [
            swap(part, ("tm", "space"), d << start) for d in range(1, 1 << take)
        ]
        start += take

    modes, spectrum = pl.pallas_call(
        functools.partial(
            tree_body,
            parts=len(parts),
            tiles=tiles,
            mode_scale=math.sqrt(width),
            value_scale=1.0 / math.sqrt(snaps * width),
            **sizes,
        ),
        out_shape=[
            jax.ShapeDtypeStruct((rank, piece), f32),
            jax.ShapeDtypeStruct((1, rank), f32),
        ],
        name="merge_tree",
    )(*parts, wide, pair, span, rows)
    return modes, spectrum.reshape(rank)


def solution(mesh):
    def local(snapshots, start_block, merge_mix):
        plan = local_fast if fits(mesh, snapshots, start_block) else local_plain
        return plan(snapshots, start_block, merge_mix)

    return jax.shard_map(
        local,
        mesh=mesh,
        in_specs=(P("tm", "space"), P("tm", None), P()),
        out_specs=(P(None, ("space", "tm")), P()),
        check_vma=False,
    )
```

```python
import functools
import math

import jax
import jax.numpy as jnp
from jax import lax
from jax.experimental import pallas as pl
from jax.experimental.pallas import tpu as pltpu
from jax.sharding import PartitionSpec as P

ITERS = 2
LANES = 128
SUBLANES = 8
EYE_LANE = 32
ELIM_BLOCK = 10
VMEM_LIMIT = 24 << 20

HIGHEST_PREC = lax.Precision.HIGHEST


def from_partner(block, axis, distance):
    count = lax.axis_size(axis)
    route = []
    for low in range(count):
        high = low | 1 << distance
        if high != low and high < count:
            route += [(low, high), (high, low)]
    return lax.ppermute(block, axis, route)


def merge_rule(gram_mat, mixing):
    weighted = jnp.dot(gram_mat, mixing, precision=HIGHEST_PREC)
    small_gram = jnp.dot(mixing.T, weighted, precision=HIGHEST_PREC)
    cholesky_low = jnp.linalg.cholesky(small_gram)
    coef_map = jax.scipy.linalg.solve_triangular(cholesky_low, mixing.T, lower=True)
    spread = jnp.dot(coef_map, gram_mat, precision=HIGHEST_PREC)
    singular = jnp.sqrt(jnp.sum(spread * spread, axis=1))
    return (coef_map, singular)


def local_plain(snapshots, start_block, merge_mix):
    width = snapshots.shape[1] * lax.axis_size("space")
    block_proj = start_block
    for rounds in range(ITERS):
        rounded = block_proj.astype(jnp.bfloat16)
        images = lax.dot_general(
            rounded, snapshots, (((0,), (0,)), ((), ())), preferred_element_type=jnp.float32
        )
        images_b = images.astype(jnp.bfloat16)
        gram_part = lax.dot_general(
            images_b, images_b, (((1,), (1,)), ((), ())), preferred_element_type=jnp.float32
        )
        proj_part = lax.dot_general(
            snapshots, images_b, (((1,), (1,)), ((), ())), preferred_element_type=jnp.float32
        )
        gram_mat, projected = lax.psum((gram_part, proj_part), "space")
        cholesky_low = jnp.linalg.cholesky(gram_mat)
        block_proj = jax.scipy.linalg.solve_triangular(cholesky_low, projected.T, lower=True).T
    singular = jnp.sqrt(jnp.sum(block_proj * block_proj, axis=0))
    basis_rows = jax.scipy.linalg.solve_triangular(
        cholesky_low, images_b.astype(jnp.float32), lower=True
    )
    factor = singular[:, None] * basis_rows
    tile_total = lax.axis_size("tm")
    depth_total = tile_total.bit_length() - 1
    tm_place = lax.axis_index("tm")
    for height in range(depth_total):
        partner = from_partner(factor, "tm", height)
        upper = tm_place >> height & 1 == 1
        first = jnp.where(upper, partner, factor)
        second = jnp.where(upper, factor, partner)
        stacked = jnp.concatenate([first, second], axis=0)
        gram_local = jnp.dot(stacked, stacked.T, precision=HIGHEST_PREC)
        gram_mat = lax.psum(gram_local, "space")
        coef_map, singular = merge_rule(gram_mat, merge_mix)
        basis_rows = jnp.dot(coef_map, stacked, precision=HIGHEST_PREC)
        factor = singular[:, None] * basis_rows
    piece_cols = basis_rows.shape[1] // tile_total
    own_cols = lax.dynamic_slice_in_dim(basis_rows, tm_place * piece_cols, piece_cols, 1)
    modes = own_cols * math.sqrt(width)
    spectrum = singular / math.sqrt(snapshots.shape[0] * width)
    return (modes, spectrum)


def mm(a, b, dims=((1,), (0,))):
    return lax.dot_general(
        a, b, (dims, ((), ())), precision=HIGHEST_PREC, preferred_element_type=jnp.float32
    )


def iota(shape, dim):
    return lax.broadcasted_iota(jnp.int32, shape, dim)


def one_hot(cond):
    return jnp.where(cond, 1.0, 0.0).astype(jnp.float32)


def block_mask(shape, row_step, col_step):
    return iota(shape, 0) // row_step == iota(shape, 1) // col_step


def roll_lanes(x, shift):
    shift %= x.shape[1]
    return pltpu.roll(x, shift, 1) if shift else x


def pad_lanes(x, lanes):
    return jnp.concatenate([x, jnp.zeros((x.shape[0], lanes - x.shape[1]), x.dtype)], axis=1)


def pad_rows(x, rows):
    if rows == x.shape[0]:
        return x
    return jnp.concatenate([x, jnp.zeros((rows - x.shape[0], x.shape[1]), x.dtype)], axis=0)


def with_eye(gram_mat, rank):
    row = iota(gram_mat.shape, 0)
    lane = iota(gram_mat.shape, 1)
    return jnp.where(lane < rank, gram_mat, one_hot((lane == row + EYE_LANE) & (row < rank)))


def exact_reciprocal(x):
    guess = pl.reciprocal(x, approx=True)
    guess = guess * (2.0 - x * guess)
    return guess * (2.0 - x * guess)


def eliminate(systems, rank):
    systems = [list(s) for s in systems]
    shape = (systems[0][0].shape[0], LANES)
    row = iota(shape, 0)
    pivots = [jnp.ones(shape, jnp.float32) for _ in systems]
    for low in range(0, rank, ELIM_BLOCK):
        high = min(low + ELIM_BLOCK, rank)
        spread = [
            [jnp.broadcast_to(s[0][:, k : k + 1], shape) for k in range(low, high)]
            for s in systems
        ]
        for k in range(low, high):
            below = row > k
            for n, s in enumerate(systems):
                cols = spread[n]
                pivot = cols[k - low][k : k + 1]
                pivots[n] = jnp.where(row == k, pivot, pivots[n])
                scale = jnp.where(below, cols[k - low] * exact_reciprocal(pivot), 0.0)
                for j in range(k - low + 1, high - low):
                    cols[j] = cols[j] - scale * cols[j][k : k + 1]
                for i, v in enumerate(s):
                    if v.shape[1] > LANES:
                        wide = jnp.concatenate([scale] * (v.shape[1] // LANES), axis=1)
                        s[i] = v - wide * v[k : k + 1]
                    else:
                        s[i] = v - scale * v[k : k + 1]
    out = []
    for n, s in enumerate(systems):
        inv = jnp.where(row < rank, lax.rsqrt(pivots[n]), 0.0)
        out.append(
            [v * jnp.concatenate([inv] * (v.shape[1] // LANES), axis=1) for v in s]
        )
    return out


def corr_body(snap_ref, corr_ref, held_ref, sems, *, chunk):
    count = snap_ref.shape[1] // chunk

    def fetch(n):
        at = (slice(None), pl.ds(n * chunk, chunk))
        return pltpu.make_async_copy(snap_ref.at[at], held_ref.at[at], sems.at[n])

    for n in range(count):
        fetch(n).start()
    for n in range(count):
        fetch(n).wait()
        block = held_ref[:, n * chunk : (n + 1) * chunk]
        term = lax.dot_general(
            block, block, (((1,), (1,)), ((), ())), preferred_element_type=jnp.float32
        )
        corr_ref[...] = term if n == 0 else corr_ref[...] + term


def head_body(*refs, rank, rank_pad):
    *corr_refs, start_ref, proj_ref, slab_ref = refs
    corr = corr_refs[0][...]
    for ref in corr_refs[1:]:
        corr = corr + ref[...]
    block_t = pad_rows(start_ref[...], LANES)
    for rounds in range(ITERS):
        rounded = block_t.astype(jnp.bfloat16).astype(jnp.float32)
        proj_t = mm(rounded[:rank_pad], corr)
        gram_mat = mm(proj_t, rounded, ((1,), (1,)))
        ((done, solved),) = eliminate([(with_eye(gram_mat, rank), proj_t)], rank)
        block_t = pad_rows(solved, LANES)
    proj_ref[...] = rounded[:rank_pad].astype(jnp.bfloat16)
    singular = jnp.sqrt(jnp.sum(solved * solved, axis=1, keepdims=True))
    factor_map = singular * done
    lane = iota(factor_map.shape, 1)
    factor_map = jnp.where((lane >= EYE_LANE) & (lane < EYE_LANE + rank), factor_map, 0.0)
    slab = jnp.zeros((SUBLANES, LANES), jnp.float32)
    for q in range(rank_pad // SUBLANES):
        part = factor_map[q * SUBLANES : (q + 1) * SUBLANES]
        slab = slab + roll_lanes(part, q * rank_pad - EYE_LANE)
    slab_ref[...] = slab


def image_body(proj_ref, slab_ref, snap_ref, *out_refs, rank, rank_pad):
    piece = snap_ref.shape[1] // len(out_refs)
    half = piece // 2
    full = rank // SUBLANES
    place = lax.axis_index("tm")
    for d, out_ref in enumerate(out_refs):
        at = pl.ds(pl.multiple_of((place ^ d) * piece, LANES), piece)
        images = jnp.dot(proj_ref[...], snap_ref[:, at], preferred_element_type=jnp.float32)
        images = images.astype(jnp.bfloat16).astype(jnp.float32)
        for q in range(full):
            out_ref[:, q * piece : (q + 1) * piece] = images[q * SUBLANES : (q + 1) * SUBLANES]
        rest = images[full * SUBLANES : rank_pad]
        low = rest[:, :half]
        high = pltpu.roll(rest[:, half:], SUBLANES // 2, 0)
        out_ref[:, full * piece : full * piece + half] = low + high
        out_ref[:, full * piece + half :] = slab_ref[...]


def mix_body(mix_ref, wide_ref, pair_ref, *, rank, rank_pad):
    mix = pad_rows(pad_lanes(mix_ref[...], LANES), LANES).T
    wide_ref[...] = jnp.zeros(wide_ref.shape, jnp.float32)
    wide_ref[0:rank, :] = mix[0:rank, :]
    wide_ref[rank_pad : rank_pad + rank, :] = mix[rank : 2 * rank, :]
    pairs = pair_ref.shape[0] // (2 * rank_pad)
    wide = wide_ref[0 : 2 * rank_pad, :]
    for n in range(pairs):
        pair_ref[n * 2 * rank_pad : (n + 1) * 2 * rank_pad, :] = roll_lanes(wide, n * rank_pad)


def gram_body(*refs, tiles, rank, rank_pad):
    piece_refs = refs[:tiles]
    pair_ref, part_ref, rows_ref, span_ref, rows_f32, map_ref = refs[tiles:]
    piece = rows_f32.shape[1]
    half = piece // 2
    full = rank // SUBLANES
    place = lax.axis_index("tm")
    lane8 = iota((SUBLANES, LANES), 1)
    row8 = iota((SUBLANES, half), 0)
    for d in range(tiles):
        tile_row = pl.multiple_of((place ^ d) * rank_pad, SUBLANES)
        ref = piece_refs[d]
        for q in range(full):
            at = pl.ds(pl.multiple_of(tile_row + q * SUBLANES, SUBLANES), SUBLANES)
            rows_f32[at, :] = ref[:, q * piece : (q + 1) * piece]
        rest = ref[:, full * piece : full * piece + half]
        at = pl.ds(pl.multiple_of(tile_row + full * SUBLANES, SUBLANES), SUBLANES)
        rows_f32[at, 0:half] = jnp.where(row8 < SUBLANES // 2, rest, 0.0)
        rest = pltpu.roll(rest, SUBLANES // 2, 0)
        rows_f32[at, half:] = jnp.where(row8 < SUBLANES // 2, rest, 0.0)
        slab = ref[:, full * piece + half :]
        for q in range(rank_pad // SUBLANES):
            at = pl.ds(pl.multiple_of(tile_row + q * SUBLANES, SUBLANES), SUBLANES)
            map_ref[at, :] = jnp.where(lane8 < rank, roll_lanes(slab, -q * rank_pad), 0.0)
    rows = rows_f32[...].astype(jnp.bfloat16)
    rows_ref[...] = rows
    gram_mat = lax.dot_general(
        rows, rows, (((1,), (1,)), ((), ())), preferred_element_type=jnp.float32
    )
    total = tiles * rank_pad
    pairs = tiles // 2
    used = pairs * rank_pad
    wide_total = -(-total // LANES) * LANES
    maps = jnp.concatenate(
        [
            roll_lanes(
                pad_lanes(map_ref[j * rank_pad : (j + 1) * rank_pad, :], wide_total), j * rank_pad
            )
            for j in range(tiles)
        ],
        axis=0,
    )
    pair = pair_ref[...]
    span = mm(pair, maps, ((0,), (0,)))[:used]
    span_ref[...] = span
    cross = mm(mm(span[:, :total], gram_mat), maps[:, :total], ((1,), (1,)))
    mixed = mm(cross, pair)
    cross = pad_lanes(cross, wide_total)
    lane = iota((rank_pad, LANES), 1)
    for n in range(pairs):
        at = slice(n * rank_pad, (n + 1) * rank_pad)
        first = roll_lanes(cross[at], -n * rank_pad)[:, :LANES]
        second = roll_lanes(cross[at], used - rank_pad - 2 * n * rank_pad)[:, :LANES]
        own = (lane >= n * rank_pad) & (lane < (n + 1) * rank_pad)
        tail = (lane >= used) & (lane < used + rank_pad)
        part_ref[at, :] = jnp.where(own, first, jnp.where(tail, second, mixed[at]))


def place_blocks(blocks, rank_pad):
    return jnp.concatenate([roll_lanes(x, n * rank_pad) for n, x in enumerate(blocks)], axis=0)


def tree_body(*refs, parts, rank, rank_pad, tiles, mode_scale, value_scale):
    part_refs = refs[:parts]
    wide_ref, pair_ref, span_ref, rows_ref, modes_ref, spectrum_ref = refs[parts:]
    part = part_refs[0][...]
    for ref in part_refs[1:]:
        part = part + ref[...]
    count = tiles // 2
    used = count * rank_pad
    lane = iota((rank_pad, LANES), 1)
    blocks = []
    for b in range(count):
        mine = part[b * rank_pad : (b + 1) * rank_pad]
        first = jnp.where(lane < rank_pad, roll_lanes(mine, -b * rank_pad), 0.0)
        second = jnp.where((lane >= used) & (lane < used + rank_pad), mine, 0.0)
        blocks.append(first + roll_lanes(second, rank_pad - used))
    own = mm(jnp.concatenate(blocks, axis=0), wide_ref[...])
    grams = [own[b * rank_pad : (b + 1) * rank_pad] for b in range(count)]
    span = span_ref[...]
    diag = block_mask(part.shape, rank_pad, rank_pad)
    full = jnp.where(diag, place_blocks(grams, rank_pad), part)
    full = jnp.where(iota(part.shape, 1) < used, full, 0.0)
    while True:
        systems = []
        for b in range(count):
            if count > 1:
                systems.append((with_eye(grams[b], rank), blocks[b]))
            else:
                systems.append((jnp.where(lane < rank, grams[b], 0.0), blocks[b], span))
        solved = eliminate(systems, rank)
        values = [jnp.sqrt(jnp.sum(s[1] * s[1], axis=1, keepdims=True)) for s in solved]
        if count == 1:
            break
        maps = []
        for b in range(count):
            scaled = roll_lanes(solved[b][0] * values[b], -EYE_LANE)
            maps.append(jnp.where(lane < rank, scaled, 0.0))
        maps = place_blocks(maps, rank_pad)
        rows_now = count * rank_pad
        count //= 2
        used = count * rank_pad
        pair = pair_ref[0:rows_now, :]
        pair = jnp.where(iota(pair.shape, 1) < used, pair, 0.0)
        step = mm(pair, maps, ((0,), (0,)))[:used]
        half_way = mm(step[:, :rows_now], full[:rows_now])
        cross = mm(half_way, pad_rows(maps, LANES), ((1,), (1,)))
        full = mm(half_way, pad_rows(step, LANES), ((1,), (1,)))
        span = mm(step[:, :rows_now], span)
        blocks = []
        grams = []
        for b in range(count):
            at = slice(b * rank_pad, (b + 1) * rank_pad)
            first = roll_lanes(cross[at], -2 * b * rank_pad)
            blocks.append(jnp.where(lane < 2 * rank_pad, first, 0.0))
            grams.append(roll_lanes(full[at], -b * rank_pad))
    coef = solved[0][2][:, : rows_ref.shape[0]] * mode_scale
    high = coef.astype(jnp.bfloat16)
    rest = coef - high.astype(jnp.float32)
    mid = rest.astype(jnp.bfloat16)
    low = (rest - mid.astype(jnp.float32)).astype(jnp.bfloat16)
    rows = rows_ref[...]
    modes = jnp.dot(high, rows, preferred_element_type=jnp.float32)
    modes = modes + jnp.dot(mid, rows, preferred_element_type=jnp.float32)
    modes = modes + jnp.dot(low, rows, preferred_element_type=jnp.float32)
    modes_ref[...] = modes[:rank]
    square = solved[0][1] * solved[0][1]
    value_row = jnp.sqrt(mm(jnp.ones((SUBLANES, LANES), jnp.float32), square, ((1,), (1,))))
    spectrum_ref[...] = value_row[0:1, 0:rank] * value_scale


def fits(mesh, snapshots, start_block):
    tiles, spaces = mesh.shape["tm"], mesh.shape["space"]
    rank = start_block.shape[1]
    rank_pad = -(-rank // SUBLANES) * SUBLANES
    snaps = snapshots.shape[0]
    piece = snapshots.shape[1] // tiles
    return (
        tiles & tiles - 1 == 0
        and spaces & spaces - 1 == 0
        and tiles >= 4
        and (tiles // 2 + 1) * rank_pad <= LANES
        and rank % SUBLANES == SUBLANES // 2
        and rank <= EYE_LANE
        and rank + EYE_LANE <= LANES
        and snaps == LANES
        and snapshots.shape[1] % tiles == 0
        and piece % (2 * LANES) == 0
    )


def swap(block, axes, distance):
    size = 1
    for axis in axes:
        size *= lax.axis_size(axis)
    return lax.ppermute(block, axes, [(i, i ^ distance) for i in range(size)])


def local_fast(snapshots, start_block, merge_mix):
    tiles, spaces = lax.axis_size("tm"), lax.axis_size("space")
    snaps, cols = snapshots.shape
    rank = start_block.shape[1]
    rank_pad = -(-rank // SUBLANES) * SUBLANES
    width = cols * spaces
    piece = cols // tiles
    pairs = tiles // 2
    total = tiles * rank_pad
    f32 = jnp.float32
    sizes = {"rank": rank, "rank_pad": rank_pad}
    wide_total = -(-total // LANES) * LANES
    bf16 = jnp.bfloat16

    def call(body, name, args, outs, in_hbm=0, out_hbm=(), scratch=(), **kwargs):
        at_hbm = pl.BlockSpec(memory_space=pltpu.HBM)
        vmem = pl.BlockSpec(memory_space=pltpu.VMEM)
        for n in range(len(args)):
            place_in = pltpu.HBM if n < in_hbm else pltpu.VMEM
            args[n] = pltpu.with_memory_space_constraint(args[n], place_in)
        shapes = [
            jax.ShapeDtypeStruct(*o) if n in out_hbm else pltpu.VMEM(*o)
            for n, o in enumerate(outs)
        ]
        return pl.pallas_call(
            functools.partial(body, **kwargs),
            in_specs=[at_hbm] * in_hbm + [vmem] * (len(args) - in_hbm),
            out_specs=[vmem] * len(outs),
            out_shape=shapes,
            scratch_shapes=list(scratch),
            compiler_params=pltpu.CompilerParams(vmem_limit_bytes=VMEM_LIMIT),
            name=name,
        )(*args)

    wide, pair = call(
        mix_body,
        "mix_maps",
        [merge_mix.T],
        [((LANES, LANES), f32), ((total, LANES), f32)],
        **sizes,
    )
    chunk = piece
    corr, held = call(
        corr_body,
        "correlation",
        [snapshots],
        [((snaps, snaps), f32), ((snaps, cols), bf16)],
        in_hbm=1,
        scratch=[pltpu.SemaphoreType.DMA((cols // chunk,))],
        chunk=chunk,
    )
    corrs = [corr] + [swap(corr, ("space",), d) for d in range(1, spaces)]
    proj, slab = call(
        head_body,
        "tile_iterations",
        [*corrs, start_block.T],
        [((rank_pad, snaps), bf16), ((SUBLANES, LANES), f32)],
        **sizes,
    )
    packed = rank * piece // SUBLANES + LANES
    pieces = call(
        image_body,
        "images",
        [proj, slab, held],
        [((SUBLANES, packed), f32)] * tiles,
        **sizes,
    )
    got = [pieces[0]] + [swap(pieces[d], ("tm",), d) for d in range(1, tiles)]
    part, rows, span = call(
        gram_body,
        "cross_gram",
        [*got, pair],
        [
            ((pairs * rank_pad, LANES), f32),
            ((total, piece), bf16),
            ((pairs * rank_pad, wide_total), f32),
        ],
        scratch=[pltpu.VMEM((total, piece), f32), pltpu.VMEM((total, LANES), f32)],
        tiles=tiles,
        **sizes,
    )
    bits = (tiles * spaces).bit_length() - 1
    start = 0
    parts = [part]
    while start < bits:
        take = 1 if (bits - start) % 2 else 2
        part = sum(parts[1:], parts[0])
        parts = [part] + [
            swap(part, ("tm", "space"), d << start) for d in range(1, 1 << take)
        ]
        start += take
    modes, spectrum = call(
        tree_body,
        "merge_tree",
        [*parts, wide, pair, span, rows],
        [((rank, piece), f32), ((1, rank), f32)],
        out_hbm=(0, 1),
        parts=len(parts),
        tiles=tiles,
        mode_scale=math.sqrt(width),
        value_scale=1.0 / math.sqrt(snaps * width),
        **sizes,
    )
    return modes, spectrum.reshape(rank)


def solution(mesh):
    def local(snapshots, start_block, merge_mix):
        plan = local_fast if fits(mesh, snapshots, start_block) else local_plain
        return plan(snapshots, start_block, merge_mix)

    return jax.shard_map(
        local,
        mesh=mesh,
        in_specs=(P("tm", "space"), P("tm", None), P()),
        out_specs=(P(None, ("space", "tm")), P()),
        check_vma=False,
    )
```

```python
import functools
import math

import jax
import jax.numpy as jnp
from jax import lax
from jax.experimental import pallas as pl
from jax.experimental.pallas import tpu as pltpu
from jax.sharding import PartitionSpec as P

ITERS = 2
LANES = 128
SUBLANES = 8
EYE_LANE = 32
ELIM_BLOCK = 10
VMEM_LIMIT = 24 << 20
NEAR_SHARE = 0.5

HIGHEST_PREC = lax.Precision.HIGHEST


def from_partner(block, axis, distance):
    count = lax.axis_size(axis)
    route = []
    for low in range(count):
        high = low | 1 << distance
        if high != low and high < count:
            route += [(low, high), (high, low)]
    return lax.ppermute(block, axis, route)


def merge_rule(gram_mat, mixing):
    weighted = jnp.dot(gram_mat, mixing, precision=HIGHEST_PREC)
    small_gram = jnp.dot(mixing.T, weighted, precision=HIGHEST_PREC)
    cholesky_low = jnp.linalg.cholesky(small_gram)
    coef_map = jax.scipy.linalg.solve_triangular(cholesky_low, mixing.T, lower=True)
    spread = jnp.dot(coef_map, gram_mat, precision=HIGHEST_PREC)
    singular = jnp.sqrt(jnp.sum(spread * spread, axis=1))
    return (coef_map, singular)


def local_plain(snapshots, start_block, merge_mix):
    width = snapshots.shape[1] * lax.axis_size("space")
    block_proj = start_block
    for _ in range(ITERS):
        rounded = block_proj.astype(jnp.bfloat16)
        images = lax.dot_general(
            rounded, snapshots, (((0,), (0,)), ((), ())), preferred_element_type=jnp.float32
        )
        images_b = images.astype(jnp.bfloat16)
        gram_part = lax.dot_general(
            images_b, images_b, (((1,), (1,)), ((), ())), preferred_element_type=jnp.float32
        )
        proj_part = lax.dot_general(
            snapshots, images_b, (((1,), (1,)), ((), ())), preferred_element_type=jnp.float32
        )
        gram_mat, projected = lax.psum((gram_part, proj_part), "space")
        cholesky_low = jnp.linalg.cholesky(gram_mat)
        block_proj = jax.scipy.linalg.solve_triangular(cholesky_low, projected.T, lower=True).T
    singular = jnp.sqrt(jnp.sum(block_proj * block_proj, axis=0))
    basis_rows = jax.scipy.linalg.solve_triangular(
        cholesky_low, images_b.astype(jnp.float32), lower=True
    )
    factor = singular[:, None] * basis_rows
    tile_total = lax.axis_size("tm")
    depth_total = tile_total.bit_length() - 1
    tm_place = lax.axis_index("tm")
    for height in range(depth_total):
        partner = from_partner(factor, "tm", height)
        upper = tm_place >> height & 1 == 1
        first = jnp.where(upper, partner, factor)
        second = jnp.where(upper, factor, partner)
        stacked = jnp.concatenate([first, second], axis=0)
        gram_local = jnp.dot(stacked, stacked.T, precision=HIGHEST_PREC)
        gram_mat = lax.psum(gram_local, "space")
        coef_map, singular = merge_rule(gram_mat, merge_mix)
        basis_rows = jnp.dot(coef_map, stacked, precision=HIGHEST_PREC)
        factor = singular[:, None] * basis_rows
    piece_cols = basis_rows.shape[1] // tile_total
    own_cols = lax.dynamic_slice_in_dim(basis_rows, tm_place * piece_cols, piece_cols, 1)
    modes = own_cols * math.sqrt(width)
    spectrum = singular / math.sqrt(snapshots.shape[0] * width)
    return (modes, spectrum)


def mm(a, b, dims=((1,), (0,))):
    return lax.dot_general(
        a, b, (dims, ((), ())), precision=HIGHEST_PREC, preferred_element_type=jnp.float32
    )


def iota(shape, dim):
    return lax.broadcasted_iota(jnp.int32, shape, dim)


def one_hot(cond):
    return jnp.where(cond, 1.0, 0.0).astype(jnp.float32)


def block_mask(shape, row_step, col_step):
    return iota(shape, 0) // row_step == iota(shape, 1) // col_step


def roll_lanes(x, shift):
    shift %= x.shape[1]
    return pltpu.roll(x, shift, 1) if shift else x


def pad_lanes(x, lanes):
    return jnp.concatenate([x, jnp.zeros((x.shape[0], lanes - x.shape[1]), x.dtype)], axis=1)


def pad_rows(x, rows):
    if rows == x.shape[0]:
        return x
    return jnp.concatenate([x, jnp.zeros((rows - x.shape[0], x.shape[1]), x.dtype)], axis=0)


def with_eye(gram_mat, rank):
    row = iota(gram_mat.shape, 0)
    lane = iota(gram_mat.shape, 1)
    return jnp.where(lane < rank, gram_mat, one_hot((lane == row + EYE_LANE) & (row < rank)))


def exact_reciprocal(x):
    guess = pl.reciprocal(x, approx=True)
    guess = guess * (2.0 - x * guess)
    return guess * (2.0 - x * guess)


def eliminate(systems, rank):
    systems = [list(s) for s in systems]
    shape = (systems[0][0].shape[0], LANES)
    row = iota(shape, 0)
    pivots = [jnp.ones(shape, jnp.float32) for _ in systems]
    for low in range(0, rank, ELIM_BLOCK):
        high = min(low + ELIM_BLOCK, rank)
        spread = [
            [jnp.broadcast_to(s[0][:, k : k + 1], shape) for k in range(low, high)]
            for s in systems
        ]
        for k in range(low, high):
            below = row > k
            for n, s in enumerate(systems):
                cols = spread[n]
                pivot = cols[k - low][k : k + 1]
                pivots[n] = jnp.where(row == k, pivot, pivots[n])
                scale = jnp.where(below, cols[k - low] * exact_reciprocal(pivot), 0.0)
                for j in range(k - low + 1, high - low):
                    cols[j] = cols[j] - scale * cols[j][k : k + 1]
                for i, v in enumerate(s):
                    if v.shape[1] > LANES:
                        wide = jnp.concatenate([scale] * (v.shape[1] // LANES), axis=1)
                        s[i] = v - wide * v[k : k + 1]
                    else:
                        s[i] = v - scale * v[k : k + 1]
    out = []
    for n, s in enumerate(systems):
        inv = jnp.where(row < rank, lax.rsqrt(pivots[n]), 0.0)
        out.append(
            [v * jnp.concatenate([inv] * (v.shape[1] // LANES), axis=1) for v in s]
        )
    return out


def corr_body(snap_ref, corr_ref, held_ref, sems, *, chunk):
    count = snap_ref.shape[1] // chunk

    def fetch(n):
        at = (slice(None), pl.ds(n * chunk, chunk))
        return pltpu.make_async_copy(snap_ref.at[at], held_ref.at[at], sems.at[n])

    for n in range(count):
        fetch(n).start()
    for n in range(count):
        fetch(n).wait()
        block = held_ref[:, n * chunk : (n + 1) * chunk]
        term = lax.dot_general(
            block, block, (((1,), (1,)), ((), ())), preferred_element_type=jnp.float32
        )
        corr_ref[...] = term if n == 0 else corr_ref[...] + term


def head_body(*refs, rank, rank_pad):
    *corr_refs, start_ref, proj_ref, slab_ref = refs
    corr = corr_refs[0][...]
    for ref in corr_refs[1:]:
        corr = corr + ref[...]
    block_t = pad_rows(start_ref[...], LANES)
    for _ in range(ITERS):
        rounded = block_t.astype(jnp.bfloat16).astype(jnp.float32)
        proj_t = mm(rounded[:rank_pad], corr)
        gram_mat = mm(proj_t, rounded, ((1,), (1,)))
        ((done, solved),) = eliminate([(with_eye(gram_mat, rank), proj_t)], rank)
        block_t = pad_rows(solved, LANES)
    proj_ref[...] = rounded[:rank_pad].astype(jnp.bfloat16)
    singular = jnp.sqrt(jnp.sum(solved * solved, axis=1, keepdims=True))
    factor_map = singular * done
    lane = iota(factor_map.shape, 1)
    factor_map = jnp.where((lane >= EYE_LANE) & (lane < EYE_LANE + rank), factor_map, 0.0)
    slab = jnp.zeros((SUBLANES, LANES), jnp.float32)
    for q in range(rank_pad // SUBLANES):
        part = factor_map[q * SUBLANES : (q + 1) * SUBLANES]
        slab = slab + roll_lanes(part, q * rank_pad - EYE_LANE)
    slab_ref[...] = slab


def pack_rows(x, rank):
    half = x.shape[1] // 2
    full = rank // SUBLANES
    parts = [x[q * SUBLANES : (q + 1) * SUBLANES] for q in range(full)]
    rest = x[full * SUBLANES :]
    parts.append(rest[:, :half] + pltpu.roll(rest[:, half:], SUBLANES // 2, 0))
    return jnp.concatenate(parts, axis=1)


def unpack_rows(packed, cols, rank):
    half = cols // 2
    full = rank // SUBLANES
    parts = [packed[:, q * cols : (q + 1) * cols] for q in range(full)]
    rest = packed[:, full * cols : full * cols + half]
    top = iota(rest.shape, 0) < SUBLANES // 2
    low = jnp.where(top, rest, 0.0)
    high = jnp.where(top, pltpu.roll(rest, SUBLANES // 2, 0), 0.0)
    parts.append(jnp.concatenate([low, high], axis=1))
    return jnp.concatenate(parts, axis=0)


def unpack_map(slab, rank, rank_pad):
    parts = [roll_lanes(slab, -q * rank_pad) for q in range(rank_pad // SUBLANES)]
    full = jnp.concatenate(parts, axis=0)
    return jnp.where(iota(full.shape, 1) < rank, full, 0.0)


def three_terms(x):
    terms = []
    for _ in range(3):
        term = x.astype(jnp.bfloat16)
        terms.append(term)
        x = x - term.astype(jnp.float32)
    return jnp.concatenate([t.astype(jnp.float32) for t in terms], axis=0).astype(jnp.bfloat16)


def times_exact(x, exact):
    rows = x.shape[0]
    out = jnp.dot(three_terms(x), exact, preferred_element_type=jnp.float32)
    return out[:rows] + (out[rows : 2 * rows] + out[2 * rows :])


def image_body(proj_ref, slab_ref, snap_ref, *out_refs, near, rank, rank_pad):
    *tile_refs, own_ref, other_ref = out_refs
    piece = snap_ref.shape[1] // len(tile_refs)
    far = rank * (piece - near) // SUBLANES
    place = lax.axis_index("tm")
    slab = slab_ref[...]
    for d, out_ref in enumerate(tile_refs):
        at = pl.ds(pl.multiple_of((place ^ d) * piece, LANES), piece)
        images = jnp.dot(proj_ref[...], snap_ref[:, at], preferred_element_type=jnp.float32)
        images = images.astype(jnp.bfloat16).astype(jnp.float32)
        out_ref[:, : rank * near // SUBLANES] = pack_rows(images[:, :near], rank)
        out_ref[:, rank * near // SUBLANES :] = slab
        pair_ref = other_ref if d & 1 else own_ref
        slot = d >> 1
        pair_ref[:, slot * far : (slot + 1) * far] = pack_rows(images[:, near:], rank)
    own_ref[:, len(tile_refs) // 2 * far :] = slab
    other_ref[:, len(tile_refs) // 2 * far :] = slab


def pair_maps(own_ref, got_ref, wide_ref, rank, rank_pad):
    lower = (lax.axis_index("tm") & 1) == 0
    first, second = wide_ref[0:rank_pad, :], wide_ref[rank_pad : 2 * rank_pad, :]
    own = unpack_map(own_ref[:, own_ref.shape[1] - LANES :], rank, rank_pad)
    got = unpack_map(got_ref[:, got_ref.shape[1] - LANES :], rank, rank_pad)
    mix_own = jnp.where(lower, first, second)
    mix_got = jnp.where(lower, second, first)
    span_own = mm(mix_own, own, ((0,), (0,)))[:rank_pad]
    span_got = mm(mix_got, got, ((0,), (0,)))[:rank_pad]
    return own, got, span_own, span_got


def merge_body(own_ref, got_ref, wide_ref, *out_refs, cols, rank, rank_pad):
    far = rank * cols // SUBLANES
    _, _, span_own, span_got = pair_maps(own_ref, got_ref, wide_ref, rank, rank_pad)
    lane = iota(span_own.shape, 1)
    span = jnp.where(lane < rank_pad, span_own, roll_lanes(span_got, rank_pad))
    span = jnp.where(lane < 2 * rank_pad, span, 0.0)
    for n, out_ref in enumerate(out_refs):
        at = slice(n * far, (n + 1) * far)
        own = unpack_rows(own_ref[:, at], cols, rank)
        got = unpack_rows(got_ref[:, at], cols, rank)
        both = jnp.concatenate([own, got], axis=0).astype(jnp.bfloat16)
        out_ref[...] = pack_rows(times_exact(span[:, : 2 * rank_pad], both), rank)


def pair_body(own_ref, got_ref, wide_ref, out_ref, *, slots, cols, rank, rank_pad):
    far = rank * cols // SUBLANES
    lower = (lax.axis_index("tm") & 1) == 0
    map_own, map_got, span_own, span_got = pair_maps(own_ref, got_ref, wide_ref, rank, rank_pad)
    gram_mat = jnp.zeros((2 * rank_pad, 2 * rank_pad), jnp.float32)
    for n in range(slots):
        at = slice(n * far, (n + 1) * far)
        own = unpack_rows(own_ref[:, at], cols, rank)
        got = unpack_rows(got_ref[:, at], cols, rank)
        both = [jnp.where(lower, own, got), jnp.where(lower, got, own)]
        both = jnp.concatenate(both, axis=0).astype(jnp.bfloat16)
        gram_mat = gram_mat + lax.dot_general(
            both, both, (((1,), (1,)), ((), ())), preferred_element_type=jnp.float32
        )
    maps = [jnp.where(lower, map_own, map_got), jnp.where(lower, map_got, map_own)]
    maps = place_blocks(maps, rank_pad)
    span = jnp.where(lower, span_own, span_got) + roll_lanes(
        jnp.where(lower, span_got, span_own), rank_pad
    )
    cross = mm(mm(span[:, : 2 * rank_pad], gram_mat), maps[:, : 2 * rank_pad], ((1,), (1,)))
    out_ref[...] = pad_lanes(cross, LANES)


def mix_body(mix_ref, wide_ref, pair_ref, *, rank, rank_pad):
    mix = pad_rows(pad_lanes(mix_ref[...], LANES), LANES).T
    wide_ref[...] = jnp.zeros(wide_ref.shape, jnp.float32)
    wide_ref[0:rank, :] = mix[0:rank, :]
    wide_ref[rank_pad : rank_pad + rank, :] = mix[rank : 2 * rank, :]
    pairs = pair_ref.shape[0] // (2 * rank_pad)
    wide = wide_ref[0 : 2 * rank_pad, :]
    for n in range(pairs):
        pair_ref[n * 2 * rank_pad : (n + 1) * 2 * rank_pad, :] = roll_lanes(wide, n * rank_pad)


def gram_body(*refs, tiles, near, far, rank, rank_pad):
    pairs = tiles // 2
    piece_refs, group_refs, refs = refs[:tiles], refs[tiles : tiles + pairs], refs[tiles + pairs :]
    cross_ref, pair_ref, part_ref, rows_ref, span_ref, merged_ref, rows_f32, map_ref = refs
    place = lax.axis_index("tm")
    packed = rank * near // SUBLANES
    for d in range(tiles):
        at = pl.ds(pl.multiple_of((place ^ d) * rank_pad, SUBLANES), rank_pad)
        rows_f32[at, :] = unpack_rows(piece_refs[d][:, :packed], near, rank)
        map_ref[at, :] = unpack_map(piece_refs[d][:, packed:], rank, rank_pad)
    group = place >> 1
    for d in range(pairs):
        at = pl.ds(pl.multiple_of((group ^ d) * rank_pad, SUBLANES), rank_pad)
        merged_ref[at, :] = unpack_rows(group_refs[d][...], far, rank)
    rows = rows_f32[...].astype(jnp.bfloat16)
    rows_ref[...] = rows
    gram_mat = lax.dot_general(
        rows, rows, (((1,), (1,)), ((), ())), preferred_element_type=jnp.float32
    )
    merged = merged_ref[...]
    outer = pad_lanes(mm(merged, merged, ((1,), (1,))), LANES)
    total = tiles * rank_pad
    used = pairs * rank_pad
    wide_total = -(-total // LANES) * LANES
    maps = jnp.concatenate(
        [
            roll_lanes(
                pad_lanes(map_ref[j * rank_pad : (j + 1) * rank_pad, :], wide_total), j * rank_pad
            )
            for j in range(tiles)
        ],
        axis=0,
    )
    pair = pair_ref[...]
    span = mm(pair, maps, ((0,), (0,)))[:used]
    span_ref[...] = span
    cross = mm(mm(span[:, :total], gram_mat), maps[:, :total], ((1,), (1,)))
    mixed = mm(cross, pair) + outer
    cross = pad_lanes(cross, wide_total)
    paired = cross_ref[...]
    lane = iota((rank_pad, LANES), 1)
    for n in range(pairs):
        at = slice(n * rank_pad, (n + 1) * rank_pad)
        mine = jnp.where(group == n, paired, 0.0)
        first = roll_lanes(cross[at], -n * rank_pad)[:, :LANES]
        first = first + roll_lanes(mine, n * rank_pad)
        second = roll_lanes(cross[at], used - rank_pad - 2 * n * rank_pad)[:, :LANES]
        second = second + roll_lanes(mine, used - rank_pad)
        own = (lane >= n * rank_pad) & (lane < (n + 1) * rank_pad)
        tail = (lane >= used) & (lane < used + rank_pad)
        part_ref[at, :] = jnp.where(own, first, jnp.where(tail, second, mixed[at]))


def place_blocks(blocks, rank_pad):
    return jnp.concatenate([roll_lanes(x, n * rank_pad) for n, x in enumerate(blocks)], axis=0)


def tree_body(*refs, parts, rank, rank_pad, tiles, mode_scale, value_scale):
    part_refs = refs[:parts]
    wide_ref, pair_ref, span_ref, rows_ref, merged_ref, modes_ref, spectrum_ref = refs[parts:]
    part = part_refs[0][...]
    for ref in part_refs[1:]:
        part = part + ref[...]
    count = tiles // 2
    used = count * rank_pad
    lane = iota((rank_pad, LANES), 1)
    blocks = []
    for b in range(count):
        mine = part[b * rank_pad : (b + 1) * rank_pad]
        first = jnp.where(lane < rank_pad, roll_lanes(mine, -b * rank_pad), 0.0)
        second = jnp.where((lane >= used) & (lane < used + rank_pad), mine, 0.0)
        blocks.append(first + roll_lanes(second, rank_pad - used))
    own = mm(jnp.concatenate(blocks, axis=0), wide_ref[...])
    grams = [own[b * rank_pad : (b + 1) * rank_pad] for b in range(count)]
    span = span_ref[...]
    lead = None
    diag = block_mask(part.shape, rank_pad, rank_pad)
    full = jnp.where(diag, place_blocks(grams, rank_pad), part)
    full = jnp.where(iota(part.shape, 1) < used, full, 0.0)
    while True:
        systems = []
        for b in range(count):
            if count > 1:
                systems.append((with_eye(grams[b], rank), blocks[b]))
            else:
                systems.append((jnp.where(lane < rank, grams[b], 0.0), blocks[b], span, lead))
        solved = eliminate(systems, rank)
        values = [jnp.sqrt(jnp.sum(s[1] * s[1], axis=1, keepdims=True)) for s in solved]
        if count == 1:
            break
        maps = []
        for b in range(count):
            scaled = roll_lanes(solved[b][0] * values[b], -EYE_LANE)
            maps.append(jnp.where(lane < rank, scaled, 0.0))
        maps = place_blocks(maps, rank_pad)
        rows_now = count * rank_pad
        count //= 2
        used = count * rank_pad
        pair = pair_ref[0:rows_now, :]
        pair = jnp.where(iota(pair.shape, 1) < used, pair, 0.0)
        step = mm(pair, maps, ((0,), (0,)))[:used]
        half_way = mm(step[:, :rows_now], full[:rows_now])
        cross = mm(half_way, pad_rows(maps, LANES), ((1,), (1,)))
        full = mm(half_way, pad_rows(step, LANES), ((1,), (1,)))
        span = mm(step[:, :rows_now], span)
        lead = step if lead is None else mm(step[:, :rows_now], lead)
        blocks = []
        grams = []
        for b in range(count):
            at = slice(b * rank_pad, (b + 1) * rank_pad)
            first = roll_lanes(cross[at], -2 * b * rank_pad)
            blocks.append(jnp.where(lane < 2 * rank_pad, first, 0.0))
            grams.append(roll_lanes(full[at], -b * rank_pad))
    rows, merged = rows_ref[...], merged_ref[...]
    near = rows.shape[1]
    coef = solved[0][2][:, : rows.shape[0]] * mode_scale
    modes_ref[:, :near] = times_exact(coef, rows)[:rank]
    coef = solved[0][3][:, : merged.shape[0]] * mode_scale
    modes_ref[:, near:] = mm(coef, merged)[:rank]
    square = solved[0][1] * solved[0][1]
    value_row = jnp.sqrt(mm(jnp.ones((SUBLANES, LANES), jnp.float32), square, ((1,), (1,))))
    spectrum_ref[...] = value_row[0:1, 0:rank] * value_scale


def fits(mesh, snapshots, start_block):
    tiles, spaces = mesh.shape["tm"], mesh.shape["space"]
    rank = start_block.shape[1]
    rank_pad = -(-rank // SUBLANES) * SUBLANES
    snaps = snapshots.shape[0]
    piece = snapshots.shape[1] // tiles
    return (
        tiles & tiles - 1 == 0
        and spaces & spaces - 1 == 0
        and tiles >= 4
        and (tiles // 2 + 1) * rank_pad <= LANES
        and rank % SUBLANES == SUBLANES // 2
        and rank <= EYE_LANE
        and rank + EYE_LANE <= LANES
        and snaps == LANES
        and snapshots.shape[1] % tiles == 0
        and piece % (2 * LANES) == 0
        and piece >= 4 * LANES
    )


def near_columns(piece):
    step = 2 * LANES
    return max(step, min(piece - step, int(piece * NEAR_SHARE / step + 0.5) * step))


def swap(block, axes, distance):
    size = 1
    for axis in axes:
        size *= lax.axis_size(axis)
    return lax.ppermute(block, axes, [(i, i ^ distance) for i in range(size)])


def local_fast(snapshots, start_block, merge_mix):
    tiles, spaces = lax.axis_size("tm"), lax.axis_size("space")
    snaps, cols = snapshots.shape
    rank = start_block.shape[1]
    rank_pad = -(-rank // SUBLANES) * SUBLANES
    width = cols * spaces
    piece = cols // tiles
    pairs = tiles // 2
    total = tiles * rank_pad
    f32 = jnp.float32
    sizes = {"rank": rank, "rank_pad": rank_pad}
    wide_total = -(-total // LANES) * LANES
    bf16 = jnp.bfloat16

    def call(body, args, outs, in_hbm=0, out_hbm=(), scratch=(), **kwargs):
        at_hbm = pl.BlockSpec(memory_space=pltpu.HBM)
        vmem = pl.BlockSpec(memory_space=pltpu.VMEM)
        for n in range(len(args)):
            place_in = pltpu.HBM if n < in_hbm else pltpu.VMEM
            args[n] = pltpu.with_memory_space_constraint(args[n], place_in)
        shapes = [
            jax.ShapeDtypeStruct(*o) if n in out_hbm else pltpu.VMEM(*o)
            for n, o in enumerate(outs)
        ]
        return pl.pallas_call(
            functools.partial(body, **kwargs),
            in_specs=[at_hbm] * in_hbm + [vmem] * (len(args) - in_hbm),
            out_specs=[vmem] * len(outs),
            out_shape=shapes,
            scratch_shapes=list(scratch),
            compiler_params=pltpu.CompilerParams(vmem_limit_bytes=VMEM_LIMIT),
        )(*args)

    wide, pair = call(
        mix_body, [merge_mix.T], [((LANES, LANES), f32), ((total, LANES), f32)], **sizes
    )
    chunk = piece
    corr, held = call(
        corr_body,
        [snapshots],
        [((snaps, snaps), f32), ((snaps, cols), bf16)],
        in_hbm=1,
        scratch=[pltpu.SemaphoreType.DMA((cols // chunk,))],
        chunk=chunk,
    )
    corrs = [corr] + [swap(corr, ("space",), d) for d in range(1, spaces)]
    proj, slab = call(
        head_body,
        [*corrs, start_block.T],
        [((rank_pad, snaps), bf16), ((SUBLANES, LANES), f32)],
        **sizes,
    )
    near = near_columns(piece)
    far = piece - near
    near_packed = rank * near // SUBLANES + LANES
    far_packed = rank * far // SUBLANES
    *pieces, own, other = call(
        image_body,
        [proj, slab, held],
        [((SUBLANES, near_packed), f32)] * tiles
        + [((SUBLANES, pairs * far_packed + LANES), f32)] * 2,
        near=near,
        **sizes,
    )
    met = swap(other, ("tm",), 1)
    got = [pieces[0]]
    for d in range(1, tiles):
        got.append(swap(pieces[d], ("tm",), d))
    groups = list(call(
        merge_body, [own, met, wide], [((SUBLANES, far_packed), f32)] * pairs, cols=far, **sizes
    ))
    for d in range(1, pairs):
        groups[d] = swap(groups[d], ("tm",), 2 * d)
    (paired,) = call(
        pair_body, [own, met, wide], [((rank_pad, LANES), f32)], slots=pairs, cols=far, **sizes
    )
    part, rows, span, merged = call(
        gram_body,
        [*got, *groups, paired, pair],
        [
            ((pairs * rank_pad, LANES), f32),
            ((total, near), bf16),
            ((pairs * rank_pad, wide_total), f32),
            ((pairs * rank_pad, far), f32),
        ],
        scratch=[pltpu.VMEM((total, near), f32), pltpu.VMEM((total, LANES), f32)],
        tiles=tiles,
        near=near,
        far=far,
        **sizes,
    )
    bits = (tiles * spaces).bit_length() - 1
    start = 0
    parts = [part]
    while start < bits:
        take = 1 if (bits - start) % 2 else 2
        part = sum(parts[1:], parts[0])
        parts = [part] + [
            swap(part, ("tm", "space"), d << start) for d in range(1, 1 << take)
        ]
        start += take
    modes, spectrum = call(
        tree_body,
        [*parts, wide, pair, span, rows, merged],
        [((rank, piece), f32), ((1, rank), f32)],
        out_hbm=(0, 1),
        parts=len(parts),
        tiles=tiles,
        mode_scale=math.sqrt(width),
        value_scale=1.0 / math.sqrt(snaps * width),
        **sizes,
    )
    return modes, spectrum.reshape(rank)


def solution(mesh):
    def local(snapshots, start_block, merge_mix):
        plan = local_fast if fits(mesh, snapshots, start_block) else local_plain
        return plan(snapshots, start_block, merge_mix)

    return jax.shard_map(
        local,
        mesh=mesh,
        in_specs=(P("tm", "space"), P("tm", None), P()),
        out_specs=(P(None, ("space", "tm")), P()),
        check_vma=False,
    )
```
